32 devices in a mesh: aa: 2 (over core), ba: 16 (over z, y, x).
Axes of the slice: x: 2, y: 2, z: 4, core: 2. Of those that a mesh axis runs over, the one named last changes fastest.
Arguments:
- queries: bfloat16 [2, 16, 192, 1024], P('aa', 'ba'), may hold values from -6 to 6
- key_rows: bfloat16 [2, 16, 192, 1024], P('aa', 'ba'), may hold values from -6 to 6
- value_rows: bfloat16 [2, 16, 192, 1024], P('aa', 'ba'), may hold values from -6 to 6
- out_proj: bfloat16 [2, 1024, 1024], P('aa', 'ba'), may hold values from -0.1875 to 0.1875
- scale_ids: int32 [16, 192], P('ba'), may hold values from 0 to 7, never falling along the last dimension, each value on 1 to 64 neighbouring positions
- residual_in: bfloat16 [16, 192, 1024], P('ba'), may hold values from -4 to 4
- cotangent: bfloat16 [16, 192, 1024], P('ba'), may hold values from -6 to 6
Outputs:
- residual_out: bfloat16 [2, 16, 192, 1024], P('aa', 'ba')
- grad_query: bfloat16 [2, 16, 192, 1024], P('aa', 'ba')
- grad_key: bfloat16 [2, 16, 192, 1024], P('aa', 'ba')
- grad_value: bfloat16 [2, 16, 192, 1024], P('aa', 'ba')
- grad_proj: float32 [2, 1024, 1024], P('aa', 'ba')
The draws below stay inside these ranges and needn't reach their ends.
Inputs may be any that keep to these rules, and one draw needn't show every extreme that they name: `scale_ids`: for each image the scale ids never fall along the tokens; every scale from 0 to 7 is present, with 1 to 64 tokens.
All inputs are finite; a program needn't handle non-finite values.
Results may differ from the reference program's by a relative error of at most 0.0086.
Values may be sent and summed in bfloat16 or wider, within the bound.
A program may use at most 64 MiB of HBM per device.

```python
import math
import jax
import jax.numpy as jnp
import numpy as np
from jax import lax

HEADS = 16
HD = 64
RES = 1024
SEQ = 192
SCALES = 8
MOST = 64
INNER = 1024
IMAGES = 16
SECTIONS = 2


def query_key_pair(key):
    seeded = jax.random.fold_in(key, 9173)
    full_shape = (SECTIONS, IMAGES, SEQ, HEADS * HD)
    queries = jnp.clip(jax.random.normal(jax.random.fold_in(seeded, 5), full_shape, jnp.float32), -5.0, 5.0)
    key_rows = jnp.clip(jax.random.normal(jax.random.fold_in(seeded, 6), full_shape, jnp.float32), -5.0, 5.0)
    return (queries, key_rows)


def draw_queries(key, part):
    return query_key_pair(key)[0].astype(jnp.bfloat16)


def draw_key_rows(key, part):
    return query_key_pair(key)[1].astype(jnp.bfloat16)


def spiked(entries, key, source, target, parts, factor):
    def block_of(dim):
        return (jnp.arange(entries.shape[dim]) // (entries.shape[dim] // parts)).reshape((-1,) + (1,) * (entries.ndim - 1 - dim))

    near = jax.random.permutation(key, parts)[block_of(target)]
    far = (block_of(target) + parts // 2) % parts
    return jnp.where((block_of(source) == near) | (block_of(source) == far), factor * entries, entries)


def steps_of(rng, dims, split, smallest, high):
    loudness = 1.0
    for position, parts in split:
        draws = jax.random.uniform(jax.random.fold_in(jax.random.fold_in(rng, 6), position), (parts,), jnp.float32, smallest / len(split), high / len(split))
        loudness = loudness * jnp.repeat(jnp.exp(draws), dims[position] // parts).reshape((-1,) + (1,) * (len(dims) - 1 - position))
    return loudness


def length_profile(amount, total, most, lean):
    weights = [(1 << 20) // math.isqrt(rank ** lean) + 1 for rank in range(2, amount + 1)]
    rest, holding = total - most - (amount - 1), [1] * (amount - 1)
    while rest > 0:
        free = [i for i in range(amount - 1) if holding[i] < most]
        whole, budget = sum([weights[i] for i in free]), rest
        for i in free:
            more = min(most - holding[i], max(1, budget * weights[i] // whole), rest)
            holding[i] = holding[i] + more
            rest = rest - more
    return np.array([most] + holding)


def uneven(stream_key, count, total, reach, lean):
    if count == 2:
        one = jax.random.randint(stream_key, (), max(1, total - reach), min(reach, total - 1) + 1)
        return jnp.stack([one, total - one])
    tallies = jnp.asarray(length_profile(count, total, reach, lean), jnp.int32)
    couples = (count - 1) // 2
    donor, receiver = tallies[1:1 + 2 * couples:2], tallies[2:2 + 2 * couples:2]
    margin = jnp.minimum(donor - 1, reach - receiver)
    moved = jax.random.randint(jax.random.fold_in(stream_key, 1), (couples,), 0, 1 << 20) % (margin + 1)
    tallies = tallies.at[1:1 + 2 * couples:2].set(donor - moved).at[2:2 + 2 * couples:2].set(receiver + moved)
    return tallies[jax.random.permutation(jax.random.fold_in(stream_key, 2), count)]


def gaussian(key, extent, scale, limit, pieces=(), held_as=jnp.bfloat16):
    entries = jax.random.normal(key, extent, jnp.float32) * scale
    if len(pieces) > 0:
        entries = steps_of(key, extent, pieces, -0.22, 0.18) * entries
    return jnp.clip(entries, min=-limit, max=limit).astype(held_as)


def bell_draw_with(key, shape, scale, reach, pieces, heavy, held_as=jnp.bfloat16):
    array = scale * jax.random.normal(key, shape, jnp.float32)
    if pieces:
        array = array * steps_of(key, shape, pieces, -0.22, 0.18)
    return jnp.clip(spiked(array, jax.random.fold_in(key, 3), *heavy), -reach, reach).astype(held_as)


def setup_inputs(seed: int = 0) -> dict:
    keys = jax.random.split(jax.random.key(seed), 8)
    queries = draw_queries(jax.random.fold_in(keys[7], 71), 0)
    key_rows = draw_key_rows(jax.random.fold_in(keys[7], 71), 0)
    value_rows = bell_draw_with(keys[2], (SECTIONS, IMAGES, SEQ, INNER), 1.0, 6.0, ((0, 2), (1, 16)), (1, 3, 16, 2.0))
    out_proj = gaussian(keys[3], (SECTIONS, INNER, RES), INNER ** -0.5, 0.1875, ((0, 2), (1, 16)))
    scale_ids = jax.vmap(lambda own: jnp.searchsorted(jnp.cumsum(uneven(own, SCALES, SEQ, MOST, 2)), jnp.arange(SEQ), side="right"))(jax.random.split(keys[4], IMAGES)).reshape((IMAGES, SEQ)).astype(jnp.int32)
    residual_in = gaussian(keys[5], (IMAGES, SEQ, RES), 0.3, 4.0, ((0, 16),))
    cotangent = gaussian(keys[6], (IMAGES, SEQ, RES), 1.0, 6.0, ((0, 16),))
    return dict(queries=queries, key_rows=key_rows, value_rows=value_rows, out_proj=out_proj, scale_ids=scale_ids, residual_in=residual_in, cotangent=cotangent)


def round_low(values):
    return lax.optimization_barrier(values.astype(jnp.bfloat16)).astype(jnp.float32)


def reference(queries, key_rows, value_rows, out_proj, scale_ids, residual_in, cotangent):
    images = scale_ids.shape[0]
    length = scale_ids.shape[1]
    score_scale = HD ** -0.5
    visible = scale_ids[:, None, :] <= scale_ids[:, :, None]
    cot_rows = cotangent.reshape(images * length, RES)

    def section_pass(running, operands):
        q_all, k_all, v_all, w_out = operands
        q_heads = q_all.reshape(images, length, HEADS, HD).astype(jnp.float32)
        k_heads = k_all.reshape(images, length, HEADS, HD).astype(jnp.float32)
        v_heads = v_all.reshape(images, length, HEADS, HD).astype(jnp.float32)
        scores = jnp.einsum("bihd,bjhd->bhij", q_heads, k_heads) * score_scale
        scores = jnp.where(visible[:, None], scores, -jnp.inf)
        row_max = jnp.max(scores, axis=-1, keepdims=True)
        lifted = jnp.exp(scores - row_max)
        attn_probs = lifted / jnp.sum(lifted, axis=-1, keepdims=True)
        probs_low = round_low(attn_probs)
        attended = jnp.einsum("bhij,bjhd->bihd", probs_low, v_heads)
        attended = attended.astype(jnp.bfloat16).reshape(images * length, INNER)
        branch = jnp.dot(attended, w_out, preferred_element_type=jnp.float32)
        running_next = running + branch.reshape(images, length, RES)
        d_attn = round_low(jnp.dot(cot_rows, w_out.T, preferred_element_type=jnp.float32))
        grad_proj = lax.dot_general(attended, cot_rows, (((0,), (0,)), ((), ())), preferred_element_type=jnp.float32) / IMAGES
        d_heads = d_attn.reshape(images, length, HEADS, HD)
        grad_value = jnp.einsum("bhij,bihd->bjhd", probs_low, d_heads)
        d_probs = jnp.einsum("bihd,bjhd->bhij", d_heads, v_heads)
        row_delta = jnp.sum(attn_probs * d_probs, axis=-1, keepdims=True)
        d_scores = round_low(attn_probs * (d_probs - row_delta) * score_scale)
        grad_query = jnp.einsum("bhij,bjhd->bihd", d_scores, k_heads)
        grad_key = jnp.einsum("bhij,bihd->bjhd", d_scores, q_heads)
        outputs = (
            running_next.astype(jnp.bfloat16),
            grad_query.reshape(images, length, INNER).astype(jnp.bfloat16),
            grad_key.reshape(images, length, INNER).astype(jnp.bfloat16),
            grad_value.reshape(images, length, INNER).astype(jnp.bfloat16),
            grad_proj,
        )
        return running_next, outputs

    start_value = residual_in.astype(jnp.float32)
    final_value, stacked = lax.scan(section_pass, start_value, (queries, key_rows, value_rows, out_proj))
    return stacked[0], stacked[1], stacked[2], stacked[3], stacked[4]
```

```python
import functools

import jax
import jax.numpy as jnp
from jax import lax
from jax.experimental import pallas as pl
from jax.experimental.pallas import tpu as pltpu
from jax.sharding import PartitionSpec as P

HD = 64


def passed_along(value, axis, by):
    devices = lax.axis_size(axis)
    pairs = [(i, i + by) for i in range(devices) if 0 <= i + by < devices]
    return lax.ppermute(value, axis, pairs)


def local(queries, key_rows, value_rows, out_proj, scale_ids, residual_in, cotangent):
    images = queries.shape[1]
    length = queries.shape[2]
    inner_width = queries.shape[3]
    head_count = inner_width // HD
    res_width = residual_in.shape[2]
    flat_rows = images * length
    score_scale = HD ** (-0.5)
    image_weight = 1.0 / (lax.axis_size("ba") * images)
    w_full = lax.all_gather(out_proj, "ba", axis=1, tiled=True)[0]
    visible = scale_ids[:, None, :] <= scale_ids[:, :, None]
    q_heads = queries[0].reshape(images, length, head_count, HD)
    k_heads = key_rows[0].reshape(images, length, head_count, HD)
    v_heads = value_rows[0].reshape(images, length, head_count, HD)
    scores = (
        jnp.einsum("bihd,bjhd->bhij", q_heads, k_heads, preferred_element_type=jnp.float32)
        * score_scale
    )
    scores = jnp.where(visible[:, None], scores, -jnp.inf)
    row_max = jnp.max(scores, axis=-1, keepdims=True)
    lifted = jnp.exp(scores - row_max)
    attn_probs = lifted / jnp.sum(lifted, axis=-1, keepdims=True)
    probs_low = attn_probs.astype(jnp.bfloat16)
    attended = jnp.einsum("bhij,bjhd->bihd", probs_low, v_heads, preferred_element_type=jnp.float32)
    attn_rows = attended.astype(jnp.bfloat16).reshape(flat_rows, inner_width)
    branch = jnp.dot(attn_rows, w_full, preferred_element_type=jnp.float32)

    def relay_step(hop_index, running):
        return branch + passed_along(running, "aa", 1)

    carried = lax.fori_loop(0, lax.axis_size("aa") - 1, relay_step, branch)
    residual_rows = residual_in.reshape(flat_rows, res_width).astype(jnp.float32) + carried
    residual_out = residual_rows.astype(jnp.bfloat16).reshape(images, length, res_width)
    cot_rows = cotangent.reshape(flat_rows, res_width)
    d_attn = lax.dot_general(
        cot_rows, w_full, (((1,), (1,)), ((), ())), preferred_element_type=jnp.float32
    ).astype(jnp.bfloat16)
    product = lax.dot_general(
        attn_rows, cot_rows, (((0,), (0,)), ((), ())), preferred_element_type=jnp.float32
    )
    grad_proj = lax.psum_scatter(product * image_weight, "ba", scatter_dimension=0, tiled=True)
    d_heads = d_attn.reshape(images, length, head_count, HD)
    grad_value = jnp.einsum(
        "bhij,bihd->bjhd", probs_low, d_heads, preferred_element_type=jnp.float32
    )
    d_probs = jnp.einsum("bihd,bjhd->bhij", d_heads, v_heads, preferred_element_type=jnp.float32)
    row_delta = jnp.sum(attn_probs * d_probs, axis=-1, keepdims=True)
    d_scores = (attn_probs * (d_probs - row_delta) * score_scale).astype(jnp.bfloat16)
    grad_query = jnp.einsum(
        "bhij,bjhd->bihd", d_scores, k_heads, preferred_element_type=jnp.float32
    )
    grad_key = jnp.einsum("bhij,bihd->bjhd", d_scores, q_heads, preferred_element_type=jnp.float32)
    return (
        residual_out[None],
        grad_query.reshape(images, length, inner_width).astype(jnp.bfloat16)[None],
        grad_key.reshape(images, length, inner_width).astype(jnp.bfloat16)[None],
        grad_value.reshape(images, length, inner_width).astype(jnp.bfloat16)[None],
        grad_proj[None],
    )

BF = jnp.bfloat16
F32 = jnp.float32
NT = (((1,), (1,)), ((), ()))
PAIR = 2 * HD


def nt(a, b):
    return lax.dot_general(a, b, NT, preferred_element_type=F32)


def mm(a, b):
    return jnp.dot(a, b, preferred_element_type=F32)


def turned(value):
    return value.astype(F32).T


def flipped(z, k):
    out, bit = z, 1
    while bit <= k:
        if k & bit:
            out = out + bit - 2 * bit * ((z // bit) % 2)
        bit *= 2
    return out


def fused(
    planes, weight,
    q_in, k_in, v_in, w_in, ids_in, res_in, cot_in,
    out_ref, gq_ref, gk_ref, gv_ref, gp_ref,
    wbuf, cotg, attg, transit, att_send, att_cols, att_rows, probs, bias, dbuf,
    prod, rs_send, rs_recv, branch, running,
    q_ref, k_ref, v_ref, ids_ref, res_ref, cot_ref, send_sems, recv_sems, load_sems, above_sems,
):
    length, inner = q_ref.shape
    res_width = cot_ref.shape[1]
    rows = w_in.shape[0]
    half, quarter = length // 2, length // 4
    scale = HD ** (-0.5)
    sections = lax.axis_size("aa")
    a, b = lax.axis_index("aa"), lax.axis_index("ba")
    x, y, z = b % 2, (b // 2) % 2, b // 4
    q = b % 4
    xn, yn = b + 1 - 2 * x, b + 2 - 4 * y
    qx, qy, qd = q + 1 - 2 * x, q + 2 - 4 * y, 3 - q
    zs = [flipped(z, k) for k in range(planes)]

    def there(dest, other=False):
        return {"aa": 1 - a if other else a, "ba": dest}

    def rows_of(start, size, step):
        return pl.ds(pl.multiple_of(start, step), size)

    w_ref = wbuf.at[rows_of(b * rows, rows, rows)]
    loads = [
        pltpu.make_async_copy(src, dst, load_sems.at[i])
        for i, (src, dst) in enumerate((
            (cot_in, cot_ref), (w_in, w_ref), (ids_in, ids_ref), (q_in, q_ref),
            (k_in, k_ref), (v_in, v_ref), (res_in, res_ref),
        ))
    ]
    for load in loads:
        load.start()

    barrier = pltpu.get_barrier_semaphore()
    columns = [there(b + 4 * (zs[k] - z)) for k in range(planes)]

    def greet(semaphore, device):
        pl.semaphore_signal(
            semaphore, inc=1, device_id=device, device_id_type=pl.DeviceIdType.MESH
        )

    for device in (there(xn), there(yn), there(b, True)):
        greet(barrier, device)
    for k in range(1, planes):
        @pl.when(zs[k] > z)
        def _(k=k):
            greet(barrier, columns[k])
    pl.semaphore_wait(barrier, 3 + z)
    for k in range(1, planes):
        @pl.when(zs[k] < z)
        def _(k=k):
            greet(above_sems.at[k], columns[k])

    count = [0]

    def remote(src, dst, device):
        i = count[0]
        count[0] += 1
        return pltpu.make_async_remote_copy(
            src_ref=src, dst_ref=dst, send_sem=send_sems.at[i], recv_sem=recv_sems.at[i],
            device_id=device, device_id_type=pl.DeviceIdType.MESH,
        )

    def shard(zk, qq, part=None):
        start = (zk * 4 + qq) * rows
        if part is None:
            return wbuf.at[rows_of(start, rows, rows)]
        return wbuf.at[rows_of(start + part * (rows // 2), rows // 2, rows // 2)]

    my_half = rows_of(a * half, half, quarter)
    part_a = rows_of(a * half, quarter, quarter)
    part_b = rows_of(a * half + quarter, quarter, quarter)
    other = there(b, True)
    to_x, to_y = there(xn), there(yn)

    cot_x = remote(cot_ref.at[my_half], cotg.at[0, my_half], to_x)
    cot_y = remote(cot_ref.at[my_half], cotg.at[1, my_half], to_y)
    cot_xo = remote(cotg.at[0, my_half], cotg.at[0, my_half], other)
    cot_yo = remote(cotg.at[1, my_half], cotg.at[1, my_half], other)
    cot_da = remote(cotg.at[0, part_a], cotg.at[2, part_a], to_y)
    cot_db = remote(cotg.at[1, part_b], cotg.at[2, part_b], to_x)
    cot_do = remote(cotg.at[2, my_half], cotg.at[2, my_half], other)
    w_z = [None] + [
        remote(w_ref, shard(z, q), there(b + 4 * (zs[k] - z))) for k in range(1, planes)
    ]
    w_x, w_y, w_a, w_b = [], [], [], []
    for k in range(planes):
        mine = w_ref if k == 0 else shard(zs[k], q)
        w_x.append(remote(mine, shard(zs[k], q), to_x))
        w_y.append(remote(mine, shard(zs[k], q), to_y))
        if k == 1:
            w_d = remote(shard(z, qd), shard(z, qd), there(b + 4 * (zs[1] - z)))
            w_a.append(w_d)
            w_b.append(w_d)
            continue
        w_a.append(remote(shard(zs[k], qx, 0), shard(zs[k], qx, 0), to_y))
        w_b.append(remote(shard(zs[k], qy, 1), shard(zs[k], qy, 1), to_x))
    low, high = pl.ds(0, half), pl.ds(half, half)
    att_x = remote(att_send.at[qx], attg.at[0], to_x)
    att_y = remote(att_send.at[qy], attg.at[1], to_y)
    att_ta = remote(att_send.at[qd, low], transit.at[0], to_x)
    att_tb = remote(att_send.at[qd, high], transit.at[1], to_y)
    att_fa = remote(transit.at[0], attg.at[2, low], to_y)
    att_fb = remote(transit.at[1], attg.at[2, high], to_x)
    rs_z = [None] + [
        remote(
            rs_send.at[rows_of(zs[k] * rows, rows, rows)], rs_recv.at[k - 1],
            there(b + 4 * (zs[k] - z)),
        )
        for k in range(1, planes)
    ]
    relay = remote(branch, running, other)
    started = []

    def go(*copies):
        for copy in copies:
            copy.start()
            started.append(copy)

    loads[0].wait()
    go(cot_x, cot_y)
    loads[1].wait()
    go(w_x[0], w_y[0])

    def to_planes(above):
        for k in range(1, planes):
            @pl.when(zs[k] > z if above else zs[k] < z)
            def _(k=k):
                if above:
                    pl.semaphore_wait(above_sems.at[k], 1)
                w_z[k].start()

    to_planes(False)
    started.extend(w_z[1:])
    loads[2].wait()
    seen = jnp.broadcast_to(ids_ref[...].astype(F32), (length, length))
    bias[...] = jnp.where(seen.T <= seen, 0.0, -jnp.inf)
    lane = lax.broadcasted_iota(jnp.int32, (1, PAIR), 1)
    ones = [jnp.where(lane // HD == h, 1.0, 0.0).astype(BF) for h in range(2)]
    scaled = [jnp.where(lane // HD == h, scale, 0.0).astype(BF) for h in range(2)]

    for load in loads[3:]:
        load.wait()

    width = 4 * HD

    def forward(zk, carry):
        unit = rows_of(zk * width, width, width)
        q4, k4 = q_ref[:, unit], k_ref[:, unit]
        v_turned = turned(v_ref[:, unit]).astype(BF)
        spans = [slice(h // 2 * PAIR, (h // 2 + 1) * PAIR) for h in range(4)]
        scores = [
            nt(k4[:, spans[h]] * scaled[h % 2], q4[:, spans[h]]) + bias[...] for h in range(4)
        ]
        shares = []
        for h in range(4):
            lifted = jnp.exp(scores[h] - jnp.max(scores[h], axis=0, keepdims=True))
            shares.append(lifted * (1.0 / jnp.sum(lifted, axis=0, keepdims=True)))
        parts = [mm(v_turned[h * HD:(h + 1) * HD], shares[h].astype(BF)) for h in range(4)]
        for h in range(4):
            att_cols[h, rows_of(zk * HD, HD, HD), :] = parts[h].astype(BF)
            probs[4 * zk + h] = shares[h]
        att_rows[:, unit] = jnp.concatenate(parts, axis=0).T.astype(BF)
        return carry

    lax.fori_loop(0, planes // 2, forward, 0)
    to_planes(True)
    lax.fori_loop(planes // 2, planes, forward, 0)
    for h in range(4):
        att_send[h] = turned(att_cols[h]).astype(BF)

    cot_x.wait_recv()
    cot_y.wait_recv()
    go(cot_xo, cot_yo)
    go(att_ta, att_tb, att_x, att_y)
    go(cot_da, cot_db)

    def pass_planes(k):
        w_z[k].wait_recv()
        go(w_x[k], w_y[k])

    def pass_diagonal(k):
        w_x[k].wait_recv()
        w_y[k].wait_recv()
        if k != 1:
            go(w_a[k], w_b[k])

    def backward(k, first):
        unit = rows_of(zs[k] * width, width, width)
        dbuf[...] = nt(cot_ref[...], wbuf[unit, :]).astype(BF)
        mine = att_rows[:, unit]

        def add(c, carry):
            tile = rows_of(c * 256, 256, 256)
            term = mm(mine, wbuf[unit, tile])
            branch[:, tile] = term if first else branch[:, tile] + term
            return carry

        lax.fori_loop(0, res_width // 256, add, 0, unroll=True)

    def grads(k):
        unit = rows_of(zs[k] * width, width, width)
        d4, q4, v4 = dbuf[...], q_ref[:, unit], v_ref[:, unit]
        k_turned = turned(k_ref[:, unit]).astype(BF)
        spans = [slice(h // 2 * PAIR, (h // 2 + 1) * PAIR) for h in range(4)]
        d_probs = [nt(v4[:, spans[h]] * ones[h % 2], d4[:, spans[h]]) for h in range(4)]
        d_scores, low = [], []
        for h in range(4):
            share = probs[4 * zs[k] + h]
            delta = jnp.sum(share * d_probs[h], axis=0, keepdims=True)
            d_scores.append((share * (d_probs[h] - delta)).astype(BF))
            low.append(share.astype(BF))
        gv = [mm(low[h], d4[:, spans[h]] * ones[h % 2]) for h in range(4)]
        gk = [mm(d_scores[h], q4[:, spans[h]] * scaled[h % 2]) for h in range(4)]
        gq = [mm(k_turned[h * HD:(h + 1) * HD], d_scores[h]) for h in range(4)]
        gv_ref[:, unit] = jnp.concatenate([gv[0] + gv[1], gv[2] + gv[3]], axis=1).astype(BF)
        gk_ref[:, unit] = jnp.concatenate([gk[0] + gk[1], gk[2] + gk[3]], axis=1).astype(BF)
        gq_ref[:, unit] = (jnp.concatenate(gq, axis=0) * scale).T.astype(BF)

    def last_piece(k):
        w_a[k].wait_recv()
        if k != 1:
            w_b[k].wait_recv()
        if k == 0:
            go(w_d)

    att_ta.wait_recv()
    att_tb.wait_recv()
    go(att_fa, att_fb)
    pass_diagonal(0)
    pass_planes(1)
    cot_da.wait_recv()
    cot_db.wait_recv()
    go(cot_do)
    for k in range(2, planes):
        pass_planes(k)
    last_piece(0)
    backward(0, True)
    for copy in (cot_xo, cot_yo, cot_do, att_x, att_y, att_fa, att_fb):
        copy.wait_recv()

    flat = [turned(attg[i]).astype(BF) for i in range(3)]

    def product(c, carry):
        tile = rows_of(c * 256, 256, 256)
        total = mm(att_cols[q], cot_ref[:, tile])
        for i in range(3):
            total = total + mm(flat[i], cotg[i, :, tile])
        total = total * weight
        prod[:, tile] = total
        rs_send[:, tile] = total.astype(BF)
        return carry

    lax.fori_loop(0, res_width // 256, product, 0)
    pass_diagonal(1)
    go(*rs_z[:0:-1])
    grads(0)
    for k in range(1, planes):
        if k + 1 < planes:
            pass_diagonal(k + 1)
        last_piece(k)
        backward(k, False)
        if k == planes - 1:
            @pl.when(a == 0)
            def _():
                relay.start()
        grads(k)
    total = prod[rows_of(z * rows, rows, rows), :]
    for k in range(1, planes):
        rs_z[k].wait_recv()
        total = total + rs_recv[k - 1].astype(F32)
    gp_ref[...] = total
    base = res_ref[...].astype(F32) + branch[...]

    @pl.when(a == 0)
    def _():
        out_ref[...] = base.astype(BF)
        relay.wait_send()

    @pl.when(a == 1)
    def _():
        relay.wait_recv()
        out_ref[...] = (base + running[...]).astype(BF)

    for copy in started:
        copy.wait_send()


def flush(*refs):
    inward, outward, sems = refs[:5], refs[5:10], refs[10]
    copies = [pltpu.make_async_copy(inward[i], outward[i], sems.at[i]) for i in range(5)]
    for copy in copies:
        copy.start()
    for copy in copies:
        copy.wait()


def fused_local(queries, key_rows, value_rows, out_proj, scale_ids, residual_in, cotangent):
    n = lax.axis_size("ba")
    length, inner = queries.shape[2:]
    res_width = residual_in.shape[2]
    rows = out_proj.shape[1]
    planes = n // 4
    copies = 7 + (planes - 1) + 4 * planes + 6 + (planes - 1) + 1
    heads = inner // HD
    wide = jax.ShapeDtypeStruct((length, inner), BF)
    shapes = [
        jax.ShapeDtypeStruct((length, res_width), BF), wide, wide, wide,
        jax.ShapeDtypeStruct((rows, res_width), F32),
    ]
    outs = pl.pallas_call(
        functools.partial(fused, planes, 1.0 / n),
        out_shape=shapes,
        in_specs=[pl.BlockSpec(memory_space=pltpu.HBM)] * 7,
        out_specs=[pl.BlockSpec(memory_space=pltpu.VMEM)] * 5,
        scratch_shapes=[
            pltpu.VMEM((inner, res_width), BF),
            pltpu.VMEM((3, length, res_width), BF),
            pltpu.VMEM((3, length, planes * rows), BF),
            pltpu.VMEM((2, length // 2, planes * rows), BF),
            pltpu.VMEM((4, length, planes * rows), BF),
            pltpu.VMEM((4, planes * rows, length), BF),
            pltpu.VMEM((length, inner), BF),
            pltpu.VMEM((heads, length, length), F32),
            pltpu.VMEM((length, length), F32),
            pltpu.VMEM((length, 4 * HD), BF),
            pltpu.VMEM((planes * rows, res_width), F32),
            pltpu.VMEM((planes * rows, res_width), BF),
            pltpu.VMEM((planes - 1, rows, res_width), BF),
            pltpu.VMEM((length, res_width), F32),
            pltpu.VMEM((length, res_width), F32),
            pltpu.VMEM((length, inner), BF),
            pltpu.VMEM((length, inner), BF),
            pltpu.VMEM((length, inner), BF),
            pltpu.VMEM((1, length), jnp.int32),
            pltpu.VMEM((length, res_width), BF),
            pltpu.VMEM((length, res_width), BF),
            pltpu.SemaphoreType.DMA((copies,)),
            pltpu.SemaphoreType.DMA((copies,)),
            pltpu.SemaphoreType.DMA((7,)),
            pltpu.SemaphoreType.REGULAR((planes,)),
        ],
        compiler_params=pltpu.CompilerParams(
            collective_id=0, has_side_effects=True, vmem_limit_bytes=50 * 1024 * 1024
        ),
        name="fused_sections",
    )(*[
        pltpu.with_memory_space_constraint(part, pltpu.HBM)
        for part in (
            queries[0, 0], key_rows[0, 0], value_rows[0, 0], out_proj[0], scale_ids,
            residual_in[0], cotangent[0],
        )
    ])
    outs = pl.pallas_call(
        flush,
        out_shape=shapes,
        in_specs=[pl.BlockSpec(memory_space=pltpu.VMEM)] * 5,
        out_specs=[pl.BlockSpec(memory_space=pltpu.HBM)] * 5,
        scratch_shapes=[pltpu.SemaphoreType.DMA((5,))],
        compiler_params=pltpu.CompilerParams(vmem_limit_bytes=8 * 1024 * 1024),
        name="flush",
    )(*outs)
    return (
        outs[0][None, None], outs[1][None, None], outs[2][None, None], outs[3][None, None],
        outs[4][None],
    )


def body_for(queries, key_rows, value_rows, out_proj, scale_ids, residual_in, cotangent):
    n, sections = lax.axis_size("ba"), lax.axis_size("aa")
    images, length, inner = queries.shape[1:]
    fits = (
        sections == 2 and images == 1 and n in (8, 16, 32)
        and out_proj.shape[1] == HD and length % 64 == 0 and residual_in.shape[2] % 256 == 0
    )
    chosen = fused_local if fits else local
    return chosen(
        queries, key_rows, value_rows, out_proj, scale_ids, residual_in, cotangent
    )


def solution(mesh):
    placed = (
        P("aa", "ba", None, None),
        P("aa", "ba", None, None),
        P("aa", "ba", None, None),
        P("aa", "ba", None),
        P("ba", None),
        P("ba", None, None),
        P("ba", None, None),
    )
    return jax.shard_map(
        body_for,
        mesh=mesh,
        in_specs=placed,
        out_specs=(
            P("aa", "ba", None, None),
            P("aa", "ba", None, None),
            P("aa", "ba", None, None),
            P("aa", "ba", None, None),
            P("aa", "ba", None),
        ),
        check_vma=False,
    )
```

```python
import functools

import jax
import jax.numpy as jnp
from jax import lax
from jax.experimental import pallas as pl
from jax.experimental.pallas import tpu as pltpu
from jax.sharding import PartitionSpec as P

HD = 64


def passed_along(value, axis, by):
    devices = lax.axis_size(axis)
    pairs = [(i, i + by) for i in range(devices) if 0 <= i + by < devices]
    return lax.ppermute(value, axis, pairs)


def local(queries, key_rows, value_rows, out_proj, scale_ids, residual_in, cotangent):
    images = queries.shape[1]
    length = queries.shape[2]
    inner_width = queries.shape[3]
    head_count = inner_width // HD
    res_width = residual_in.shape[2]
    flat_rows = images * length
    score_scale = HD ** (-0.5)
    image_weight = 1.0 / (lax.axis_size("ba") * images)
    w_full = lax.all_gather(out_proj, "ba", axis=1, tiled=True)[0]
    visible = scale_ids[:, None, :] <= scale_ids[:, :, None]
    q_heads = queries[0].reshape(images, length, head_count, HD)
    k_heads = key_rows[0].reshape(images, length, head_count, HD)
    v_heads = value_rows[0].reshape(images, length, head_count, HD)
    scores = (
        jnp.einsum("bihd,bjhd->bhij", q_heads, k_heads, preferred_element_type=jnp.float32)
        * score_scale
    )
    scores = jnp.where(visible[:, None], scores, -jnp.inf)
    row_max = jnp.max(scores, axis=-1, keepdims=True)
    lifted = jnp.exp(scores - row_max)
    attn_probs = lifted / jnp.sum(lifted, axis=-1, keepdims=True)
    probs_low = attn_probs.astype(jnp.bfloat16)
    attended = jnp.einsum("bhij,bjhd->bihd", probs_low, v_heads, preferred_element_type=jnp.float32)
    attn_rows = attended.astype(jnp.bfloat16).reshape(flat_rows, inner_width)
    branch = jnp.dot(attn_rows, w_full, preferred_element_type=jnp.float32)

    def relay_step(hop_index, running):
        return branch + passed_along(running, "aa", 1)

    carried = lax.fori_loop(0, lax.axis_size("aa") - 1, relay_step, branch)
    residual_rows = residual_in.reshape(flat_rows, res_width).astype(jnp.float32) + carried
    residual_out = residual_rows.astype(jnp.bfloat16).reshape(images, length, res_width)
    cot_rows = cotangent.reshape(flat_rows, res_width)
    d_attn = lax.dot_general(
        cot_rows, w_full, (((1,), (1,)), ((), ())), preferred_element_type=jnp.float32
    ).astype(jnp.bfloat16)
    product = lax.dot_general(
        attn_rows, cot_rows, (((0,), (0,)), ((), ())), preferred_element_type=jnp.float32
    )
    grad_proj = lax.psum_scatter(product * image_weight, "ba", scatter_dimension=0, tiled=True)
    d_heads = d_attn.reshape(images, length, head_count, HD)
    grad_value = jnp.einsum(
        "bhij,bihd->bjhd", probs_low, d_heads, preferred_element_type=jnp.float32
    )
    d_probs = jnp.einsum("bihd,bjhd->bhij", d_heads, v_heads, preferred_element_type=jnp.float32)
    row_delta = jnp.sum(attn_probs * d_probs, axis=-1, keepdims=True)
    d_scores = (attn_probs * (d_probs - row_delta) * score_scale).astype(jnp.bfloat16)
    grad_query = jnp.einsum(
        "bhij,bjhd->bihd", d_scores, k_heads, preferred_element_type=jnp.float32
    )
    grad_key = jnp.einsum("bhij,bihd->bjhd", d_scores, q_heads, preferred_element_type=jnp.float32)
    return (
        residual_out[None],
        grad_query.reshape(images, length, inner_width).astype(jnp.bfloat16)[None],
        grad_key.reshape(images, length, inner_width).astype(jnp.bfloat16)[None],
        grad_value.reshape(images, length, inner_width).astype(jnp.bfloat16)[None],
        grad_proj[None],
    )

BF = jnp.bfloat16
F32 = jnp.float32
NT = (((1,), (1,)), ((), ()))
PAIR = 2 * HD


def nt(a, b):
    return lax.dot_general(a, b, NT, preferred_element_type=F32)


def mm(a, b):
    return jnp.dot(a, b, preferred_element_type=F32)


def turned(value):
    return value.astype(F32).T


def flipped(z, k):
    out, bit = z, 1
    while bit <= k:
        if k & bit:
            out = out + bit - 2 * bit * ((z // bit) % 2)
        bit *= 2
    return out


def fused(
    planes, weight,
    q_in, k_in, v_in, w_in, ids_in, res_in, cot_in,
    out_ref, gq_ref, gk_ref, gv_ref, gp_ref,
    wbuf, cotg, attg, apair, att_send, att_cols, probs, bias, d_cols, d_send, d_recv,
    prod, rs_send, rs_recv, branch, paired, b_send, b_recv, b_relay, running,
    q_ref, k_ref, v_ref, ids_ref, res_ref, cot_ref, send_sems, recv_sems, load_sems, above_sems,
    rs_sems,
):
    length, inner = q_ref.shape
    res_width = cot_ref.shape[1]
    rows = w_in.shape[0]
    half, quarter = length // 2, length // 4
    chunks = res_width // 256
    scale = HD ** (-0.5)
    sections = lax.axis_size("aa")
    a, b = lax.axis_index("aa"), lax.axis_index("ba")
    x, y, z = b % 2, (b // 2) % 2, b // 4
    q = b % 4
    xn, yn = b + 1 - 2 * x, b + 2 - 4 * y
    pn, gn = xn + a * (yn - xn), yn + a * (xn - yn)
    qp, qg, qd = pn % 4, gn % 4, 3 - q
    zs = [flipped(z, k) for k in range(planes)]

    def there(dest, other=False):
        return {"aa": 1 - a if other else a, "ba": dest}

    def rows_of(start, size, step):
        return pl.ds(pl.multiple_of(start, step), size)

    def shard(slot, zk):
        return wbuf.at[slot, rows_of(zk * rows, rows, rows)]

    w_ref = shard(0, z)
    loads = [
        pltpu.make_async_copy(src, dst, load_sems.at[i])
        for i, (src, dst) in enumerate((
            (cot_in, cot_ref), (w_in, w_ref), (ids_in, ids_ref), (q_in, q_ref),
            (k_in, k_ref), (v_in, v_ref), (res_in, res_ref),
        ))
    ]
    for load in loads:
        load.start()

    barrier = pltpu.get_barrier_semaphore()
    columns = [there(b + 4 * (zs[k] - z)) for k in range(planes)]

    def greet(semaphore, device):
        pl.semaphore_signal(
            semaphore, inc=1, device_id=device, device_id_type=pl.DeviceIdType.MESH
        )

    for device in (there(xn), there(yn), there(b, True)):
        greet(barrier, device)
    for k in range(1, planes):
        @pl.when(zs[k] > z)
        def _(k=k):
            greet(barrier, columns[k])
    pl.semaphore_wait(barrier, 3 + z)
    for k in range(1, planes):
        @pl.when(zs[k] < z)
        def _(k=k):
            greet(above_sems.at[k], columns[k])

    count = [0]

    def remote(src, dst, device):
        i = count[0]
        count[0] += 1
        return pltpu.make_async_remote_copy(
            src_ref=src, dst_ref=dst, send_sem=send_sems.at[i], recv_sem=recv_sems.at[i],
            device_id=device, device_id_type=pl.DeviceIdType.MESH,
        )

    my_half = rows_of(a * half, half, quarter)
    part_a = rows_of(a * half, quarter, quarter)
    part_b = rows_of(a * half + quarter, quarter, quarter)
    other = there(b, True)
    to_x, to_y = there(xn), there(yn)
    to_p, to_g = there(pn), there(gn)

    cot_x = remote(cot_ref.at[my_half], cotg.at[0, my_half], to_x)
    cot_y = remote(cot_ref.at[my_half], cotg.at[1, my_half], to_y)
    cot_xo = remote(cotg.at[0, my_half], cotg.at[0, my_half], other)
    cot_yo = remote(cotg.at[1, my_half], cotg.at[1, my_half], other)
    cot_da = remote(cotg.at[0, part_a], cotg.at[2, part_a], to_y)
    cot_db = remote(cotg.at[1, part_b], cotg.at[2, part_b], to_x)
    cot_do = remote(cotg.at[2, my_half], cotg.at[2, my_half], other)
    w_z = [None] + [remote(w_ref, shard(0, z), columns[k]) for k in range(1, planes)]
    w_g = [remote(shard(0, zs[k]), shard(1, zs[k]), to_g) for k in range(planes)]
    att_p = remote(att_send.at[qp], attg.at[a], to_p)
    att_d = remote(att_send.at[qd], apair, to_p)
    att_g = remote(att_send.at[qg], attg.at[1 - a], to_g)
    att_f = remote(apair, attg.at[2], to_g)
    d_p = [remote(d_send.at[i], d_recv.at[i], to_p) for i in range(2)]
    b_p = [remote(b_send.at[c], b_recv.at[c], to_p) for c in range(chunks)]
    b_o = [remote(b_recv.at[c], b_relay.at[c], other) for c in range(chunks)]
    rs_out = []
    for dest in range(planes):
        k = flipped(z, dest)
        slot = jnp.maximum(k - 1, 0)
        rs_out.append(pltpu.make_async_remote_copy(
            src_ref=rs_send.at[pl.ds(dest * rows, rows)], dst_ref=rs_recv.at[slot],
            send_sem=rs_sems.at[0, slot], recv_sem=rs_sems.at[1, slot],
            device_id=there(b + 4 * (dest - z)), device_id_type=pl.DeviceIdType.MESH,
        ))
    rs_in = [
        pltpu.make_async_remote_copy(
            src_ref=rs_send.at[pl.ds(0, rows)], dst_ref=rs_recv.at[k - 1],
            send_sem=rs_sems.at[0, k - 1], recv_sem=rs_sems.at[1, k - 1],
            device_id=columns[k], device_id_type=pl.DeviceIdType.MESH,
        )
        for k in range(1, planes)
    ]
    relay = remote(branch, running, other)
    started = []

    def go(*copies):
        for copy in copies:
            copy.start()
            started.append(copy)

    loads[0].wait()
    go(cot_x, cot_y)
    loads[1].wait()

    def to_planes(above):
        for k in range(1, planes):
            @pl.when(zs[k] > z if above else zs[k] < z)
            def _(k=k):
                if above:
                    pl.semaphore_wait(above_sems.at[k], 1)
                w_z[k].start()

    to_planes(False)
    started.extend(w_z[1:])
    loads[2].wait()
    seen = jnp.broadcast_to(ids_ref[...].astype(F32), (length, length))
    bias[...] = jnp.where(seen.T <= seen, 0.0, -jnp.inf)
    lane = lax.broadcasted_iota(jnp.int32, (1, PAIR), 1)
    ones = [jnp.where(lane // HD == h, 1.0, 0.0).astype(BF) for h in range(2)]
    scaled = [jnp.where(lane // HD == h, scale, 0.0).astype(BF) for h in range(2)]

    for load in loads[3:]:
        load.wait()

    width = 4 * HD

    def forward(zk, carry):
        unit = rows_of(zk * width, width, width)
        q4, k4 = q_ref[:, unit], k_ref[:, unit]
        v_turned = turned(v_ref[:, unit]).astype(BF)
        spans = [slice(h // 2 * PAIR, (h // 2 + 1) * PAIR) for h in range(4)]
        scores = [
            nt(k4[:, spans[h]] * scaled[h % 2], q4[:, spans[h]]) + bias[...] for h in range(4)
        ]
        shares = []
        for h in range(4):
            lifted = jnp.exp(scores[h] - jnp.max(scores[h], axis=0, keepdims=True))
            shares.append(lifted * (1.0 / jnp.sum(lifted, axis=0, keepdims=True)))
        parts = [mm(v_turned[h * HD:(h + 1) * HD], shares[h].astype(BF)) for h in range(4)]
        for h in range(4):
            att_cols[h, rows_of(zk * HD, HD, HD), :] = parts[h].astype(BF)
            probs[4 * zk + h] = shares[h]
        return carry

    lax.fori_loop(0, planes // 2, forward, 0)
    to_planes(True)
    lax.fori_loop(planes // 2, planes, forward, 0)
    for h in range(4):
        att_send[h] = turned(att_cols[h]).astype(BF)
    go(att_d, att_p, att_g)

    cot_x.wait_recv()
    cot_y.wait_recv()
    go(cot_xo, cot_yo)
    go(cot_da, cot_db)

    def pass_plane(k):
        w_z[k].wait_recv()
        go(w_g[k])

    def near(c, carry):
        tile = rows_of(c * 256, 256, 256)
        total = mm(att_cols[q], cot_ref[:, tile])
        for i in range(2):
            total = total + mm(flat[i], cotg[i, :, tile])
        prod[:, tile] = total
        return carry

    def far(c, carry):
        tile = rows_of(c * 256, 256, 256)
        total = (prod[:, tile] + mm(flat[2], cotg[2, :, tile])) * weight
        prod[:, tile] = total
        rs_send[:, tile] = total.astype(BF)
        return carry

    def backward(i):
        block, mine, theirs = wbuf.at[i], att_send[(q, qg)[i]], (attg.at[a], apair)[i][...]
        d_send[i] = nt(cotg[a], block[...]).astype(BF)
        go(d_p[i])
        for c in range(chunks):
            tile = slice(c * 256, (c + 1) * 256)
            term = mm(theirs, block[:, tile])
            if i == 0:
                paired[:, tile] = term
            else:
                b_send[c] = (paired[:, tile] + term).astype(BF)
                go(b_p[c])
        for c in range(chunks):
            tile = slice(c * 256, (c + 1) * 256)
            term = mm(mine, block[:, tile])
            branch[:, tile] = term if i == 0 else branch[:, tile] + term
        d_cols[(q, qg)[i]] = nt(block[...], cot_ref[...]).astype(BF)

    def grads(zk):
        unit = rows_of(zk * width, width, width)
        rows_in = rows_of(zk * HD, HD, HD)
        q4, v4 = q_ref[:, unit], v_ref[:, unit]
        k_turned = turned(k_ref[:, unit]).astype(BF)
        spans = [slice(h // 2 * PAIR, (h // 2 + 1) * PAIR) for h in range(4)]
        d_pairs = [
            jnp.concatenate([d_cols[2 * i, rows_in, :], d_cols[2 * i + 1, rows_in, :]], axis=0)
            for i in range(2)
        ]
        d_probs = [mm(v4[:, spans[h]] * ones[h % 2], d_pairs[h // 2]) for h in range(4)]
        d_scores, low = [], []
        for h in range(4):
            share = probs[4 * zk + h]
            delta = jnp.sum(share * d_probs[h], axis=0, keepdims=True)
            d_scores.append((share * (d_probs[h] - delta)).astype(BF))
            low.append(share.astype(BF))
        gv = [nt(low[h], d_pairs[h // 2]) for h in range(4)]
        gk = [mm(d_scores[h], q4[:, spans[h]] * scaled[h % 2]) for h in range(4)]
        gq = [mm(k_turned[h * HD:(h + 1) * HD], d_scores[h]) for h in range(4)]
        left = lane < HD
        gv = [jnp.where(left, gv[2 * i], gv[2 * i + 1]) for i in range(2)]
        gv_ref[:, unit] = jnp.concatenate(gv, axis=1).astype(BF)
        gk_ref[:, unit] = jnp.concatenate([gk[0] + gk[1], gk[2] + gk[3]], axis=1).astype(BF)
        gq_ref[:, unit] = (jnp.concatenate(gq, axis=0) * scale).T.astype(BF)

    def later_planes():
        for k in range(2, planes):
            pass_plane(k)
        backward(0)

    att_d.wait_recv()
    go(att_f)
    go(w_g[0])
    pass_plane(1)
    for copy in (cot_xo, cot_yo, att_p, att_g):
        copy.wait_recv()
    flat = [turned(attg[i]).astype(BF) for i in range(2)]
    lax.fori_loop(0, chunks, near, 0)
    cot_da.wait_recv()
    cot_db.wait_recv()
    go(cot_do)
    count_started = len(started)

    @pl.when(z >= planes // 2)
    def _():
        later_planes()

    del started[count_started:]
    cot_do.wait_recv()
    att_f.wait_recv()
    flat.append(turned(attg[2]).astype(BF))
    lax.fori_loop(0, chunks, far, 0)
    for dest in range(planes):
        @pl.when(dest != z)
        def _(dest=dest):
            rs_out[dest].start()

    @pl.when(z < planes // 2)
    def _():
        later_planes()

    d_p[0].wait_recv()
    d_cols[qp] = turned(d_recv[0]).astype(BF)
    for k in range(planes):
        w_g[k].wait_recv()
    backward(1)

    @pl.when(a == 0)
    def _():
        relay.start()

    d_p[1].wait_recv()
    d_cols[qd] = turned(d_recv[1]).astype(BF)

    def grads_step(zk, carry):
        grads(zk)
        return carry

    lax.fori_loop(0, planes, grads_step, 0)
    total = prod[rows_of(z * rows, rows, rows), :]
    for k in range(1, planes):
        rs_in[k - 1].wait_recv()
        total = total + rs_recv[k - 1].astype(F32)
    gp_ref[...] = total

    @pl.when(a == 1)
    def _():
        relay.wait_recv()

    for c in range(chunks):
        tile = slice(c * 256, (c + 1) * 256)
        b_p[c].wait_recv()
        base = res_ref[:, tile].astype(F32) + branch[:, tile] + b_recv[c].astype(F32)

        @pl.when(a == 0)
        def _(c=c, tile=tile, base=base):
            b_o[c].start()
            out_ref[:, tile] = base.astype(BF)

        @pl.when(a == 1)
        def _(c=c, tile=tile, base=base):
            b_o[c].wait_recv()
            out_ref[:, tile] = (base + running[:, tile] + b_relay[c].astype(F32)).astype(BF)

    @pl.when(a == 0)
    def _():
        relay.wait_send()
        for copy in b_o:
            copy.wait_send()

    for copy in started + rs_in:
        copy.wait_send()


def flush(*refs):
    inward, outward, sems = refs[:5], refs[5:10], refs[10]
    copies = [pltpu.make_async_copy(inward[i], outward[i], sems.at[i]) for i in range(5)]
    for copy in copies:
        copy.start()
    for copy in copies:
        copy.wait()


def fused_local(queries, key_rows, value_rows, out_proj, scale_ids, residual_in, cotangent):
    n = lax.axis_size("ba")
    length, inner = queries.shape[2:]
    res_width = residual_in.shape[2]
    rows = out_proj.shape[1]
    planes = n // 4
    chunks = res_width // 256
    copies = 7 + (planes - 1) + planes + 4 + 2 + 2 * chunks + 1
    heads = inner // HD
    wide = jax.ShapeDtypeStruct((length, inner), BF)
    shapes = [
        jax.ShapeDtypeStruct((length, res_width), BF), wide, wide, wide,
        jax.ShapeDtypeStruct((rows, res_width), F32),
    ]
    outs = pl.pallas_call(
        functools.partial(fused, planes, 1.0 / n),
        out_shape=shapes,
        in_specs=[pl.BlockSpec(memory_space=pltpu.HBM)] * 7,
        out_specs=[pl.BlockSpec(memory_space=pltpu.VMEM)] * 5,
        scratch_shapes=[
            pltpu.VMEM((2, planes * rows, res_width), BF),
            pltpu.VMEM((3, length, res_width), BF),
            pltpu.VMEM((3, length, planes * rows), BF),
            pltpu.VMEM((length, planes * rows), BF),
            pltpu.VMEM((4, length, planes * rows), BF),
            pltpu.VMEM((4, planes * rows, length), BF),
            pltpu.VMEM((heads, length, length), F32),
            pltpu.VMEM((length, length), F32),
            pltpu.VMEM((4, planes * rows, length), BF),
            pltpu.VMEM((2, length, planes * rows), BF),
            pltpu.VMEM((2, length, planes * rows), BF),
            pltpu.VMEM((planes * rows, res_width), F32),
            pltpu.VMEM((planes * rows, res_width), BF),
            pltpu.VMEM((planes - 1, rows, res_width), BF),
            pltpu.VMEM((length, res_width), F32),
            pltpu.VMEM((length, res_width), F32),
            pltpu.VMEM((chunks, length, 256), BF),
            pltpu.VMEM((chunks, length, 256), BF),
            pltpu.VMEM((chunks, length, 256), BF),
            pltpu.VMEM((length, res_width), F32),
            pltpu.VMEM((length, inner), BF),
            pltpu.VMEM((length, inner), BF),
            pltpu.VMEM((length, inner), BF),
            pltpu.VMEM((1, length), jnp.int32),
            pltpu.VMEM((length, res_width), BF),
            pltpu.VMEM((length, res_width), BF),
            pltpu.SemaphoreType.DMA((copies,)),
            pltpu.SemaphoreType.DMA((copies,)),
            pltpu.SemaphoreType.DMA((7,)),
            pltpu.SemaphoreType.REGULAR((planes,)),
            pltpu.SemaphoreType.DMA((2, planes - 1)),
        ],
        compiler_params=pltpu.CompilerParams(
            collective_id=0, has_side_effects=True, vmem_limit_bytes=50 * 1024 * 1024
        ),
        name="fused_sections",
    )(*[
        pltpu.with_memory_space_constraint(part, pltpu.HBM)
        for part in (
            queries[0, 0], key_rows[0, 0], value_rows[0, 0], out_proj[0], scale_ids,
            residual_in[0], cotangent[0],
        )
    ])
    outs = pl.pallas_call(
        flush,
        out_shape=shapes,
        in_specs=[pl.BlockSpec(memory_space=pltpu.VMEM)] * 5,
        out_specs=[pl.BlockSpec(memory_space=pltpu.HBM)] * 5,
        scratch_shapes=[pltpu.SemaphoreType.DMA((5,))],
        compiler_params=pltpu.CompilerParams(vmem_limit_bytes=8 * 1024 * 1024),
        name="flush",
    )(*outs)
    return (
        outs[0][None, None], outs[1][None, None], outs[2][None, None], outs[3][None, None],
        outs[4][None],
    )


def body_for(queries, key_rows, value_rows, out_proj, scale_ids, residual_in, cotangent):
    n, sections = lax.axis_size("ba"), lax.axis_size("aa")
    images, length, inner = queries.shape[1:]
    fits = (
        sections == 2 and images == 1 and n in (8, 16, 32)
        and out_proj.shape[1] == HD and length % 64 == 0 and residual_in.shape[2] % 256 == 0
    )
    chosen = fused_local if fits else local
    return chosen(
        queries, key_rows, value_rows, out_proj, scale_ids, residual_in, cotangent
    )


def solution(mesh):
    placed = (
        P("aa", "ba", None, None),
        P("aa", "ba", None, None),
        P("aa", "ba", None, None),
        P("aa", "ba", None),
        P("ba", None),
        P("ba", None, None),
        P("ba", None, None),
    )
    return jax.shard_map(
        body_for,
        mesh=mesh,
        in_specs=placed,
        out_specs=(
            P("aa", "ba", None, None),
            P("aa", "ba", None, None),
            P("aa", "ba", None, None),
            P("aa", "ba", None, None),
            P("aa", "ba", None),
        ),
        check_vma=False,
    )
```
